256 devices in a mesh: data: 256 (over z, y, x, core).
Axes of the slice: x: 4, y: 4, z: 8, core: 2. Of those that a mesh axis runs over, the one named last changes fastest.
Arguments:
- act_in: bfloat16 [8192, 896], P('data')
- grad_top: bfloat16 [8192, 896], P('data')
- w_up: bfloat16 [2, 896, 4864], P(None, None, 'data')
- w_down: bfloat16 [2, 4864, 896], P(None, 'data')
- proj_up: bfloat16 [2, 896, 128], replicated
- proj_down: bfloat16 [2, 896, 128], replicated
- mom_up: float32 [2, 128, 4864], P(None, None, 'data')
- var_up: float32 [2, 128, 4864], P(None, None, 'data')
- mom_down: float32 [2, 4864, 128], P(None, 'data')
- var_down: float32 [2, 4864, 128], P(None, 'data')
Outputs:
- output 1: bfloat16 [2, 896, 4864], P(None, None, 'data')
- output 2: bfloat16 [2, 4864, 896], P(None, 'data')
- output 3: float32 [2, 128, 4864], P(None, None, 'data')
- output 4: float32 [2, 128, 4864], P(None, None, 'data')
- output 5: float32 [2, 4864, 128], P(None, 'data')
- output 6: float32 [2, 4864, 128], P(None, 'data')
All inputs are finite; a program needn't handle non-finite values.
Results may differ from the reference program's by a relative error of at most 0.00400308.
Values are sent between devices in bfloat16 or wider.
A program may use at most 768 MiB of HBM per device.

```python
import jax
import jax.numpy as jnp

TOK_DEV = 32
DEVICES = 256
D = 896
FF = 4864
RANK = 128
LAYERS = 2
STEP = 3

TOKENS = TOK_DEV * DEVICES
BETA_ONE = 0.9
BETA_TWO = 0.999
ADAM_EPS = 1e-8
STEP_SIZE = 0.05 / RANK ** 0.5
GRAD_SCALE = 0.5


def orthonormal(key, rows, cols):
    gauss_mat = jax.random.normal(key, (LAYERS, rows, cols), jnp.float32)
    return jnp.linalg.qr(gauss_mat)[0]


def setup_inputs(seed: int = 0) -> dict:
    key_list = jax.random.split(jax.random.key(seed), 10)
    mom_scale = (1.0 - BETA_ONE ** (STEP - 1)) * GRAD_SCALE
    var_scale = (1.0 - BETA_TWO ** (STEP - 1)) * GRAD_SCALE ** 2
    act_in = jax.random.normal(key_list[0], (TOKENS, D), jnp.float32)
    grad_top = jax.random.normal(key_list[1], (TOKENS, D), jnp.float32) * TOKENS ** -0.5
    w_up = jax.random.normal(key_list[2], (LAYERS, D, FF), jnp.float32) * D ** -0.5
    w_down = jax.random.normal(key_list[3], (LAYERS, FF, D), jnp.float32) * FF ** -0.5
    proj_up = orthonormal(key_list[4], D, RANK)
    proj_down = orthonormal(key_list[5], D, RANK)
    mom_up = jax.random.normal(key_list[6], (LAYERS, RANK, FF), jnp.float32) * mom_scale
    var_up = (0.25 + jax.random.normal(key_list[7], (LAYERS, RANK, FF), jnp.float32) ** 2) * var_scale
    mom_down = jax.random.normal(key_list[8], (LAYERS, FF, RANK), jnp.float32) * mom_scale
    var_down = (0.25 + jax.random.normal(key_list[9], (LAYERS, FF, RANK), jnp.float32) ** 2) * var_scale
    return dict(
        act_in=act_in.astype(jnp.bfloat16),
        grad_top=grad_top.astype(jnp.bfloat16),
        w_up=w_up.astype(jnp.bfloat16),
        w_down=w_down.astype(jnp.bfloat16),
        proj_up=proj_up.astype(jnp.bfloat16),
        proj_down=proj_down.astype(jnp.bfloat16),
        mom_up=mom_up,
        var_up=var_up,
        mom_down=mom_down,
        var_down=var_down,
    )


def adam_direction(grad_proj, moment, second):
    mom_new = BETA_ONE * moment + (1.0 - BETA_ONE) * grad_proj
    second_new = BETA_TWO * second + (1.0 - BETA_TWO) * grad_proj * grad_proj
    mom_hat = mom_new / (1.0 - BETA_ONE ** STEP)
    second_hat = second_new / (1.0 - BETA_TWO ** STEP)
    return mom_hat / (jnp.sqrt(second_hat) + ADAM_EPS), mom_new, second_new


def reference(act_in, grad_top, w_up, w_down, proj_up, proj_down, mom_up, var_up, mom_down, var_down):
    hidden = [act_in]
    pre_acts = []
    post_acts = []
    for layer_idx in range(LAYERS):
        pre_act = jnp.dot(hidden[-1], w_up[layer_idx], preferred_element_type=jnp.float32)
        post_act = jax.nn.gelu(pre_act).astype(jnp.bfloat16)
        mlp_out = jnp.dot(post_act, w_down[layer_idx], preferred_element_type=jnp.float32)
        hidden.append((hidden[-1].astype(jnp.float32) + mlp_out).astype(jnp.bfloat16))
        pre_acts.append(pre_act)
        post_acts.append(post_act)
    grad_cur = grad_top
    new_up = [None] * LAYERS
    new_down = [None] * LAYERS
    mom_up_new = [None] * LAYERS
    var_up_new = [None] * LAYERS
    mom_down_new = [None] * LAYERS
    var_down_new = [None] * LAYERS
    for layer_idx in reversed(range(LAYERS)):
        grad_down = jnp.dot(post_acts[layer_idx].T, grad_cur, preferred_element_type=jnp.float32)
        d_post = jnp.dot(grad_cur, w_down[layer_idx].T, preferred_element_type=jnp.float32)
        _, gelu_back = jax.vjp(jax.nn.gelu, pre_acts[layer_idx])
        d_pre = gelu_back(d_post)[0].astype(jnp.bfloat16)
        grad_up = jnp.dot(hidden[layer_idx].T, d_pre, preferred_element_type=jnp.float32)
        if layer_idx > 0:
            back_in = jnp.dot(d_pre, w_up[layer_idx].T, preferred_element_type=jnp.float32)
            grad_cur = (grad_cur.astype(jnp.float32) + back_in).astype(jnp.bfloat16)
        proj_up_f = proj_up[layer_idx].astype(jnp.float32)
        proj_down_f = proj_down[layer_idx].astype(jnp.float32)
        red_up = jnp.dot(proj_up_f.T, grad_up)
        red_down = jnp.dot(grad_down, proj_down_f)
        dir_up, mom_a, var_a = adam_direction(red_up, mom_up[layer_idx], var_up[layer_idx])
        dir_down, mom_b, var_b = adam_direction(red_down, mom_down[layer_idx], var_down[layer_idx])
        up_step = jnp.dot(proj_up_f, dir_up)
        down_step = jnp.dot(dir_down, proj_down_f.T)
        new_up[layer_idx] = (w_up[layer_idx].astype(jnp.float32) - STEP_SIZE * up_step).astype(jnp.bfloat16)
        new_down[layer_idx] = (w_down[layer_idx].astype(jnp.float32) - STEP_SIZE * down_step).astype(jnp.bfloat16)
        mom_up_new[layer_idx] = mom_a
        var_up_new[layer_idx] = var_a
        mom_down_new[layer_idx] = mom_b
        var_down_new[layer_idx] = var_b
    return (jnp.stack(new_up), jnp.stack(new_down), jnp.stack(mom_up_new), jnp.stack(var_up_new), jnp.stack(mom_down_new), jnp.stack(var_down_new))
```

```python
import jax
import jax.numpy as jnp
from jax import lax
from jax.experimental import pallas as pl
from jax.experimental.pallas import tpu as pltpu
from jax.sharding import PartitionSpec as P

BETA_ONE = 0.9
BETA_TWO = 0.999
ADAM_EPS = 1e-8
STEP = 3
STEP_SCALE = 0.05

NZ, NY, NX, NC = 8, 4, 4, 2
SLOTS = NY * NZ
SHARE = 19
ROWS = 40
KA = 512
BF16 = jnp.bfloat16
F32 = jnp.float32
GELU_C = 0.7978845608028654
GELU_A = 0.044715


def slot(dy, dz):
    return (dy % NY) * NZ + dz % NZ


def z_forward(part, dy, dz):
    dz %= NZ
    far_from_right = {0: part == 0, 1: True, 2: False, 3: False}[dy % NY]
    if dz == 0:
        return [("zm", 1), ("zp", NZ - 1)]
    if dz < 4:
        if dz < 3 or far_from_right:
            return [("zm", dz + 1)]
    elif dz > 4:
        if dz > 5 or not far_from_right:
            return [("zp", dz - 1)]
    return []


def y_forward(part, dy, dz):
    dy %= NY
    far_from_right = dz % 2 == 0
    if dy == 0:
        return [("ym", 1), ("yp", NY - 1)]
    if dy == 1 and far_from_right:
        return [("ym", 2)]
    if dy == 3 and not far_from_right:
        return [("yp", 2)]
    return []


def forwards(part, dy, dz):
    out = []
    if part == 0:
        if dy == 0:
            out += [(d, dy, n) for d, n in z_forward(part, dy, dz)]
        out += [(d, n, dz) for d, n in y_forward(part, dy, dz)]
    else:
        if dz == 0:
            out += [(d, n, dz) for d, n in y_forward(part, dy, dz)]
        out += [(d, dy, n) for d, n in z_forward(part, dy, dz)]
    return out


def wave_of(dy, dz):
    return min(dy, NY - dy) + min(dz, NZ - dz)


def check_tree():
    for part in (0, 1):
        got = set()
        for dy in range(NY):
            for dz in range(NZ):
                for _, ny, nz in forwards(part, dy, dz):
                    assert (ny % NY, nz % NZ) not in got
                    assert wave_of(ny % NY, nz % NZ) == wave_of(dy, dz) + 1
                    got.add((ny % NY, nz % NZ))
        assert len(got) == SLOTS - 1 and (0, 0) not in got


check_tree()


def nt(a, b):
    return lax.dot_general(a, b, (((1,), (1,)), ((), ())), preferred_element_type=F32)


def tn(a, b):
    return lax.dot_general(a, b, (((0,), (0,)), ((), ())), preferred_element_type=F32)


def nn(a, b):
    return lax.dot_general(a, b, (((1,), (0,)), ((), ())), preferred_element_type=F32)


def split(a):
    hi = a.astype(BF16)
    lo = (a - hi.astype(F32)).astype(BF16)
    return hi, lo


def kernel(h_ref, g_ref, xown_ref, pu_ref, pd_ref, m_ref, v_ref,
           w_out, m_out, v_out,
           xa, xb, h0, g1, h1, g0, xo, pq, mv, vv,
           act0, act1, gp0, dz0, dz1,
           part, rd, lbuf, rbuf, mid,
           rr, rmid, rl, rrt, zq, zbuf, res,
           wst, mst, vst,
           loc_sem, w_send, w_recv, ag_send, ag_recv, rs_send, rs_recv, r_send, r_recv, z_send, z_recv, out_sem):
    model = h_ref.shape[1]
    rank = pu_ref.shape[2]
    tok = h_ref.shape[0]
    group = NC * NX * tok
    step_size = STEP_SCALE / rank ** 0.5
    me = lax.axis_index("data")
    core = lax.rem(me, NC)
    x = lax.rem(lax.div(me, NC), NX)
    y = lax.rem(lax.div(me, NC * NX), NY)
    z = lax.div(me, NC * NX * NY)

    def dev(zz, yy, xx, cc):
        return ((lax.rem(zz, NZ) * NY + lax.rem(yy, NY)) * NX + lax.rem(xx, NX)) * NC + cc

    partner = dev(z, y, x, 1 - core)
    nbr = {
        "xp": dev(z, y, x + 1, core), "xm": dev(z, y, x + NX - 1, core),
        "yp": dev(z, y + 1, x, core), "ym": dev(z, y + NY - 1, x, core),
        "zp": dev(z + 1, y, x, core), "zm": dev(z + NZ - 1, y, x, core),
    }
    zdev = [None] + [dev(z + k, y, x, core) for k in range(1, NZ)]

    def remote(src, dst, ssem, rsem, target):
        return pltpu.make_async_remote_copy(
            src_ref=src, dst_ref=dst, send_sem=ssem, recv_sem=rsem,
            device_id=(target,), device_id_type=pl.DeviceIdType.MESH)

    local = []

    def stage(src, dst):
        copy = pltpu.make_async_copy(src, dst, loc_sem.at[len(local)])
        copy.start()
        local.append(copy)

    for layer in (0, 1):
        stage(xown_ref.at[layer, :, pl.ds(0, KA)], xa.at[layer, 0])
        stage(xown_ref.at[layer, :, pl.ds(KA, model - KA)], xb.at[layer, 0])
    stage(h_ref, h0.at[0, 0])
    stage(g_ref, g1.at[0, 0])
    stage(xown_ref, xo)
    for layer in (0, 1):
        stage(pu_ref.at[layer], pq.at[layer, :, pl.ds(0, rank)])
        stage(pd_ref.at[layer], pq.at[layer, :, pl.ds(rank, rank)])
    stage(m_ref, mv)
    stage(v_ref, vv)

    barrier = pltpu.get_barrier_semaphore()
    partners = [partner, nbr["xp"], nbr["xm"], nbr["yp"], nbr["ym"]] + zdev[1:]
    for target in partners:
        pl.semaphore_signal(barrier, inc=1, device_id=(target,), device_id_type=pl.DeviceIdType.MESH)
    pl.semaphore_wait(barrier, len(partners))
    for copy in local:
        copy.wait()

    wparts = (xa, xb)

    def w_issue(layer, prt, dy, dz):
        buf = wparts[prt]
        for direction, ny, nz in forwards(prt, dy, dz):
            remote(buf.at[layer, slot(dy, dz)], buf.at[layer, slot(ny, nz)],
                   w_send.at[layer, prt], w_recv.at[layer, prt, slot(ny, nz)], nbr[direction]).start()

    def w_own(layer):
        w_issue(layer, 0, 0, 0)
        w_issue(layer, 1, 0, 0)

    def w_wave(layer, wave):
        for dy in range(NY):
            for dz in range(NZ):
                if wave_of(dy, dz) == wave:
                    for prt in (0, 1):
                        s = slot(dy, dz)
                        buf = wparts[prt]
                        remote(buf.at[layer, s], buf.at[layer, s], w_send.at[layer, prt],
                               w_recv.at[layer, prt, s], partner).wait_recv()
                        w_issue(layer, prt, dy, dz)

    def w_drain(layer):
        for prt in (0, 1):
            buf = wparts[prt]
            remote(buf.at[layer, pl.ds(1, SLOTS - 1)], buf.at[layer, pl.ds(1, SLOTS - 1)],
                   w_send.at[layer, prt], w_recv.at[layer, prt, 0], partner).wait_send()

    half = tok // 2
    drains = []

    class Gather:
        def __init__(self, buf, index):
            self.buf, self.index = buf, index

        def copy(self, k, src, dst, target):
            return remote(src, dst, ag_send.at[self.index, k], ag_recv.at[self.index, k], target)

        def go(self, k, src, dst, target):
            copy = self.copy(k, src, dst, target)
            copy.start()
            drains.append(copy)

        def arrived(self, k, ref):
            self.copy(k, ref, ref, partner).wait_recv()

        def start(self):
            b = self.buf
            self.go(0, b.at[0, 0], b.at[0, 3], nbr["xp"])
            self.go(1, b.at[0, 0], b.at[0, 1], nbr["xm"])
            self.go(2, b.at[0, 0], b.at[1, 0], partner)

        def middle(self):
            b = self.buf
            lo, hi = pl.ds(0, half), pl.ds(half, half)
            self.arrived(0, b.at[0, 3])
            self.go(3, b.at[0, 3, lo], b.at[0, 2, lo], nbr["xp"])
            self.go(5, b.at[0, 3], b.at[1, 3], partner)
            self.arrived(1, b.at[0, 1])
            self.go(4, b.at[0, 1, hi], b.at[0, 2, hi], nbr["xm"])
            self.go(6, b.at[0, 1], b.at[1, 1], partner)

        def last(self):
            b = self.buf
            lo, hi = pl.ds(0, half), pl.ds(half, half)
            self.arrived(3, b.at[0, 2, lo])
            self.arrived(4, b.at[0, 2, hi])
            self.go(7, b.at[0, 2], b.at[1, 2], partner)

        def finish(self):
            b = self.buf
            self.arrived(2, b.at[1, 0])
            self.arrived(5, b.at[1, 3])
            self.arrived(6, b.at[1, 1])
            self.arrived(7, b.at[1, 2])

    class Reduce:
        def __init__(self, index):
            self.index = index

        def copy(self, k, src, dst, target):
            return remote(src, dst, rs_send.at[self.index, k], rs_recv.at[self.index, k], target)

        def go(self, k, src, dst, target):
            copy = self.copy(k, src, dst, target)
            copy.start()
            drains.append(copy)

        def arrived(self, k, ref):
            self.copy(k, ref, ref, partner).wait_recv()

        def to_partner(self):
            i = self.index
            self.go(0, part.at[i, 1], rd.at[i], partner)

        def ring(self):
            i = self.index
            lo, hi = pl.ds(0, half), pl.ds(half, half)
            self.arrived(0, rd.at[i])
            part[i, 0, 2] = part[i, 0, 2] + rd[i, 2]
            self.go(1, part.at[i, 0, 2, lo], mid.at[i, lo], nbr["xp"])
            self.go(2, part.at[i, 0, 2, hi], mid.at[i, hi], nbr["xm"])
            part[i, 0, 1] = part[i, 0, 1] + rd[i, 1]
            self.go(3, part.at[i, 0, 1, hi], lbuf.at[i, hi], nbr["xp"])
            part[i, 0, 3] = part[i, 0, 3] + rd[i, 3]
            self.go(4, part.at[i, 0, 3, lo], rbuf.at[i, lo], nbr["xm"])
            part[i, 0, 0] = part[i, 0, 0] + rd[i, 0]

        def ring_second(self):
            i = self.index
            lo, hi = pl.ds(0, half), pl.ds(half, half)
            self.arrived(1, mid.at[i, lo])
            part[i, 0, 1, lo] = part[i, 0, 1, lo] + mid[i, lo]
            self.go(5, part.at[i, 0, 1, lo], lbuf.at[i, lo], nbr["xp"])
            self.arrived(2, mid.at[i, hi])
            part[i, 0, 3, hi] = part[i, 0, 3, hi] + mid[i, hi]
            self.go(6, part.at[i, 0, 3, hi], rbuf.at[i, hi], nbr["xm"])

        def total(self):
            i = self.index
            lo, hi = pl.ds(0, half), pl.ds(half, half)
            self.arrived(3, lbuf.at[i, hi])
            self.arrived(4, rbuf.at[i, lo])
            self.arrived(5, lbuf.at[i, lo])
            self.arrived(6, rbuf.at[i, hi])
            return part[i, 0, 0] + lbuf[i] + rbuf[i]

    class Scatter:
        def __init__(self, layer):
            self.layer = layer

        def copy(self, k, src, dst, target):
            return remote(src, dst, r_send.at[self.layer, k], r_recv.at[self.layer, k], target)

        def go(self, k, src, dst, target):
            copy = self.copy(k, src, dst, target)
            copy.start()
            drains.append(copy)

        def arrived(self, k, ref):
            self.copy(k, ref, ref, partner).wait_recv()

        def ring(self):
            i = self.layer
            lo, hi = pl.ds(0, NZ // 2), pl.ds(NZ // 2, NZ // 2)
            self.go(0, rr.at[i, 2, lo], rmid.at[i, lo], nbr["yp"])
            self.go(1, rr.at[i, 2, hi], rmid.at[i, hi], nbr["ym"])
            self.go(2, rr.at[i, 1, hi], rl.at[i, hi], nbr["yp"])
            self.go(3, rr.at[i, 3, lo], rrt.at[i, lo], nbr["ym"])

        def ring_second(self):
            i = self.layer
            lo, hi = pl.ds(0, NZ // 2), pl.ds(NZ // 2, NZ // 2)
            self.arrived(0, rmid.at[i, lo])
            rr[i, 1, lo] = rr[i, 1, lo] + rmid[i, lo]
            self.go(4, rr.at[i, 1, lo], rl.at[i, lo], nbr["yp"])
            self.arrived(1, rmid.at[i, hi])
            rr[i, 3, hi] = rr[i, 3, hi] + rmid[i, hi]
            self.go(5, rr.at[i, 3, hi], rrt.at[i, hi], nbr["ym"])

        def along_z(self):
            i = self.layer
            lo, hi = pl.ds(0, NZ // 2), pl.ds(NZ // 2, NZ // 2)
            self.arrived(2, rl.at[i, hi])
            self.arrived(3, rrt.at[i, lo])
            self.arrived(4, rl.at[i, lo])
            self.arrived(5, rrt.at[i, hi])
            zq[i] = rr[i, 0] + rl[i] + rrt[i]
            for k in (4, 3, 5, 2, 6, 1, 7):
                copy = remote(zq.at[i, k], zbuf.at[i, NZ - k], z_send.at[i, k], z_recv.at[i, NZ - k], zdev[k])
                copy.start()
                drains.append(copy)

        def total(self):
            i = self.layer
            out = zq[i, 0]
            for k in range(1, NZ):
                remote(zbuf.at[i, k], zbuf.at[i, k], z_send.at[i, k], z_recv.at[i, k], partner).wait_recv()
                out = out + zbuf[i, k]
            return out

    rows = SLOTS * ROWS
    CH = 640
    per = CH // ROWS

    def xrows(layer, i):
        a = xa[layer, pl.ds(i * per, per)].reshape(CH, KA)
        b = xb[layer, pl.ds(i * per, per)].reshape(CH, model - KA)
        return a, b

    def against(x2, acts):
        return nt(x2[0], acts[:, :KA]) + nt(x2[1], acts[:, KA:])

    def row_in_slot():
        r = lax.broadcasted_iota(jnp.int32, (CH, group), 0)
        return lax.rem(r, ROWS)

    def chunks(body):
        def step(i, carry):
            body(i)
            return carry
        lax.fori_loop(0, rows // CH, step, 0)

    def gelu_pair(zt):
        sq = zt * zt
        t = jnp.tanh(GELU_C * (zt + GELU_A * (zt * sq)))
        half_one = 0.5 * (1.0 + t)
        value = zt * half_one
        slope = half_one + 0.5 * zt * (1.0 - t * t) * (GELU_C * (1.0 + 3.0 * GELU_A * sq))
        return value, slope

    def to_down(v):
        r = row_in_slot()
        keep = jnp.logical_and(r >= SHARE, r < 2 * SHARE)
        return jnp.where(keep, pltpu.roll(v, SHARE, 0), 0.0)

    def to_up(v):
        return pltpu.roll(v, CH - SHARE, 0)

    def mask_up(v):
        return jnp.where(row_in_slot() < SHARE, v, 0.0)

    def block(i):
        return pl.ds(pl.multiple_of(i * CH, CH), CH)

    def products(act_ref, layer, out_index):
        def body(j):
            for q in range(1, -1, -1):
                pass
        for cc in (1, 0):
            toks = pl.ds(cc * (group // 2), group // 2)
            lhs = act_ref[:, toks]
            a = xa[layer].reshape(rows, KA)
            b = xb[layer].reshape(rows, model - KA)
            part[out_index, cc, :, :, pl.ds(0, KA)] = tn(lhs, a).reshape(NX, tok, KA)
            part[out_index, cc, :, :, pl.ds(KA, model - KA)] = tn(lhs, b).reshape(NX, tok, model - KA)
            if cc == 1:
                Reduce(out_index).to_partner()

    def flat(ref):
        return ref[...].reshape(group, model)

    def project(layer, h_ref2, g_ref2):
        hp = nn(flat(h_ref2), pq[layer])[:, :rank]
        gq = nn(flat(g_ref2), pq[layer])[:, rank:]
        return jnp.concatenate(split(hp), axis=1), jnp.concatenate(split(gq), axis=1)

    gather_h, gather_g = Gather(h0, 0), Gather(g1, 1)
    w_own(0)
    gather_h.start()
    w_own(1)
    gather_g.start()
    w_wave(0, 1)
    gather_h.middle()
    w_wave(0, 2)
    w_wave(1, 1)
    gather_h.last()
    gather_g.middle()
    w_wave(0, 3)
    w_wave(1, 2)
    gather_g.last()
    gather_h.finish()
    w_wave(0, 4)
    w_wave(1, 3)
    gather_g.finish()
    w_wave(0, 5)
    w_wave(1, 4)
    w_wave(0, 6)

    acts = flat(h0)

    @chunks
    def _(i):
        zt = against(xrows(0, i), flat(h0))
        value, slope = gelu_pair(zt)
        gp0[block(i), :] = slope
        act0[block(i), :] = to_down(value).astype(BF16)

    products(act0, 0, 0)
    w_wave(1, 5)
    reduce0 = Reduce(0)
    reduce0.ring()
    reduce0.ring_second()
    w_wave(1, 6)
    h1[0, 0] = (h0[0, 0].astype(F32) + reduce0.total()).astype(BF16)
    gather1 = Gather(h1, 2)
    gather1.start()
    gather1.middle()
    gather1.last()
    gather1.finish()

    @chunks
    def _(i):
        x2 = xrows(1, i)
        value, slope = gelu_pair(against(x2, flat(h1)))
        act1[block(i), :] = to_down(value).astype(BF16)
        dpost = to_up(against(x2, flat(g1)))
        dz1[block(i), :] = mask_up(slope * dpost).astype(BF16)

    products(dz1, 1, 1)
    reduce1 = Reduce(1)

    def projected(layer, dz_ref, act_ref, h_ref2, g_ref2):
        hp, gq = project(layer, h_ref2, g_ref2)

        @chunks
        def _(i):
            both = nn(dz_ref[block(i), :], hp) + nn(act_ref[block(i), :], gq)
            both = both[:, :rank] + both[:, rank:]
            both = both.reshape(per // NZ, NZ, ROWS, rank)
            rr[layer, pl.ds(i * (per // NZ), per // NZ)] = both

    reduce1.ring()
    reduce1.ring_second()
    projected(1, dz1, act1, h1, g1)
    scatter1 = Scatter(1)
    scatter1.ring()
    g0[0, 0] = (g1[0, 0].astype(F32) + reduce1.total()).astype(BF16)
    gather0 = Gather(g0, 3)
    gather0.start()
    scatter1.ring_second()
    gather0.middle()
    gather0.last()
    gather0.finish()

    @chunks
    def _(i):
        dpost = to_up(against(xrows(0, i), flat(g0)))
        dz0[block(i), :] = mask_up(gp0[block(i), :] * dpost).astype(BF16)

    projected(0, dz0, act0, h0, g0)
    scatter0 = Scatter(0)
    scatter0.ring()
    scatter1.along_z()

    def update(layer, red):
        mom = BETA_ONE * mv[layer] + (1.0 - BETA_ONE) * red
        var = BETA_TWO * vv[layer] + (1.0 - BETA_TWO) * red * red
        direction = (mom / (1.0 - BETA_ONE ** STEP)) / (jnp.sqrt(var / (1.0 - BETA_TWO ** STEP)) + ADAM_EPS)
        mst[layer] = mom
        vst[layer] = var
        r = lax.broadcasted_iota(jnp.int32, (ROWS, rank), 0)
        up = jnp.where(r < SHARE, direction, 0.0)
        down = jnp.where(r >= SHARE, direction, 0.0)
        both = jnp.concatenate([up, down], axis=1)
        hi, lo = split(both)
        change = nt(jnp.concatenate([hi, lo], axis=0), pq[layer])
        change = change[:ROWS] + change[ROWS:]
        wst[layer] = (xo[layer].astype(F32) - step_size * change).astype(BF16)

    scatter0.ring_second()
    scatter0.along_z()
    update(1, scatter1.total())
    update(0, scatter0.total())

    outs = [(wst, w_out), (mst, m_out), (vst, v_out)]
    copies = [pltpu.make_async_copy(src, dst, out_sem.at[k]) for k, (src, dst) in enumerate(outs)]
    for copy in copies:
        copy.start()
    w_drain(0)
    w_drain(1)
    for copy in drains:
        copy.wait_send()
    for copy in copies:
        copy.wait()


def fused_step(act_in, grad_top, xown, proj_up, proj_down, mom, var):
    tok, model = act_in.shape
    layers, _, rank = proj_up.shape
    kb = model - KA
    group = NC * NX * tok
    rows = SLOTS * ROWS
    dma = pltpu.SemaphoreType.DMA
    anyspace = pl.BlockSpec(memory_space=pl.ANY)
    vm = pltpu.VMEM
    blk = (NC, NX, tok, model)
    scratch = [
        vm((2, SLOTS, ROWS, KA), BF16), vm((2, SLOTS, ROWS, kb), BF16),
        vm(blk, BF16), vm(blk, BF16), vm(blk, BF16), vm(blk, BF16),
        vm((2, ROWS, model), BF16), vm((2, model, 2 * rank), BF16), vm((2, ROWS, rank), F32), vm((2, ROWS, rank), F32),
        vm((rows, group), BF16), vm((rows, group), BF16), vm((rows, group), F32), vm((rows, group), BF16), vm((rows, group), BF16),
        vm((2,) + blk, F32), vm((2, NX, tok, model), F32), vm((2, tok, model), F32), vm((2, tok, model), F32), vm((2, tok, model), F32),
        vm((2, NY, NZ, ROWS, rank), F32), vm((2, NZ, ROWS, rank), F32), vm((2, NZ, ROWS, rank), F32), vm((2, NZ, ROWS, rank), F32),
        vm((2, NZ, ROWS, rank), F32), vm((2, NZ, ROWS, rank), F32), vm((2, ROWS, rank), F32),
        vm((2, ROWS, model), BF16), vm((2, ROWS, rank), F32), vm((2, ROWS, rank), F32),
        dma((13,)), dma((2, 2)), dma((2, 2, SLOTS)), dma((4, 8)), dma((4, 8)), dma((2, 7)), dma((2, 7)),
        dma((2, 6)), dma((2, 6)), dma((2, NZ)), dma((2, NZ)), dma((3,)),
    ]
    return pl.pallas_call(
        kernel,
        name="galore_step",
        out_shape=(jax.ShapeDtypeStruct((2, ROWS, model), BF16), jax.ShapeDtypeStruct((2, ROWS, rank), F32),
                   jax.ShapeDtypeStruct((2, ROWS, rank), F32)),
        in_specs=[anyspace] * 7,
        out_specs=(anyspace,) * 3,
        scratch_shapes=scratch,
        compiler_params=pltpu.CompilerParams(collective_id=0, has_side_effects=True, vmem_limit_bytes=48 * 1024 * 1024),
    )(act_in, grad_top, xown, proj_up, proj_down, mom, var)


def solution(mesh):
    def pack(up, down):
        up = up.transpose(0, 2, 1)
        pad = jnp.zeros((up.shape[0], ROWS - 2 * SHARE, up.shape[2]), up.dtype)
        return jnp.concatenate([up, down, pad], axis=1)

    def unpack(packed):
        return packed[:, :SHARE].transpose(0, 2, 1), packed[:, SHARE:2 * SHARE]

    def device_step(act_in, grad_top, w_up, w_down, proj_up, proj_down, mom_up, var_up, mom_down, var_down):
        w_new, m_new, v_new = fused_step(act_in, grad_top, pack(w_up, w_down), proj_up, proj_down,
                                         pack(mom_up, mom_down), pack(var_up, var_down))
        new_up, new_down = unpack(w_new)
        new_mom_up, new_mom_down = unpack(m_new)
        new_var_up, new_var_down = unpack(v_new)
        return new_up, new_down, new_mom_up, new_var_up, new_mom_down, new_var_down

    tok_spec = P("data", None)
    col_spec = P(None, None, "data")
    row_spec = P(None, "data", None)
    return jax.shard_map(
        device_step,
        mesh=mesh,
        in_specs=(tok_spec, tok_spec, col_spec, row_spec, P(), P(), col_spec, col_spec, row_spec, row_spec),
        out_specs=(col_spec, row_spec, col_spec, col_spec, row_spec, row_spec),
        check_vma=False,
    )
```

```python
import heapq

import jax
import jax.numpy as jnp
from jax import lax
from jax.experimental import pallas as pl
from jax.experimental.pallas import tpu as pltpu
from jax.sharding import PartitionSpec as P

BETA_ONE = 0.9
BETA_TWO = 0.999
ADAM_EPS = 1e-8
STEP = 3
STEP_SCALE = 0.05

NZ, NY, NX, NC = 8, 4, 4, 2
SLOTS = NY * NZ
SHARE = 19
ROWS = 40
PARTS = ((0, 256, True, 0), (256, 256, True, 1), (512, 256, False, 0), (768, 128, False, 1))
BF16 = jnp.bfloat16
F32 = jnp.float32
GELU_C = 0.7978845608028654
GELU_A = 0.044715


def slot(dy, dz):
    return (dy % NY) * NZ + dz % NZ


def forwards(prt, dy, dz):
    _, _, z_first, variant = PARTS[prt]
    dy %= NY
    dz %= NZ
    far_z = (variant == 0) if z_first else (dy < 2) == (variant == 0)
    far_y = (dz + variant) % 2 == 0
    along_z, along_y = [], []
    if dz == 0:
        along_z = [("zm", dy, 1), ("zp", dy, NZ - 1)]
    elif dz < 4 and (dz < 3 or far_z):
        along_z = [("zm", dy, dz + 1)]
    elif dz > 4 and (dz > 5 or not far_z):
        along_z = [("zp", dy, dz - 1)]
    if dy == 0:
        along_y = [("ym", 1, dz), ("yp", NY - 1, dz)]
    elif (dy == 1 and far_y):
        along_y = [("ym", 2, dz)]
    elif (dy == 3 and not far_y):
        along_y = [("yp", 2, dz)]
    if z_first:
        return (along_z if dy == 0 else []) + along_y
    return (along_y if dz == 0 else []) + along_z


def path_left(prt, dy, dz):
    nxt = forwards(prt, dy, dz)
    return 1 + max(path_left(prt, ny, nz) for _, ny, nz in nxt) if nxt else 0


def weight_order(latency=1.75, rate=46600.0, late=6.0):
    queues = {d: [] for d in ("zp", "zm", "yp", "ym")}
    free = dict.fromkeys(queues, 0.0)
    events, out, count = [], [], 0

    def push(t, kind, data):
        nonlocal count
        heapq.heappush(events, (t, count, kind, data))
        count += 1

    def arrive(t, layer, prt, dy, dz):
        nonlocal count
        for d, ny, nz in forwards(prt, dy, dz):
            queues[d].append((layer, -path_left(prt, ny, nz), count, prt, dy, dz, ny, nz))
            count += 1
            push(t, "kick", d)

    push(0.0, "own", 0)
    push(late, "own", 1)
    while events:
        t, _, kind, data = heapq.heappop(events)
        if kind == "own":
            for prt in range(len(PARTS)):
                arrive(t, data, prt, 0, 0)
        elif kind == "kick":
            if free[data] <= t + 1e-9 and queues[data]:
                queues[data].sort()
                layer, _, _, prt, dy, dz, ny, nz = queues[data].pop(0)
                out.append((t, "send", layer, prt, dy, dz, data, ny, nz))
                free[data] = t + 2 * ROWS * PARTS[prt][1] / rate
                push(free[data], "kick", data)
                push(free[data] + latency, "arrive", (layer, prt, ny, nz))
        else:
            out.append((t, "wait", *data, None, None, None))
            arrive(t, *data)
    for layer in (0, 1):
        for prt in range(len(PARTS)):
            got = [e[4:6] for e in out if e[1:4] == ("wait", layer, prt)]
            assert len(got) == len(set(got)) == SLOTS - 1 and (0, 0) not in got
    return out


ORDER = weight_order()


def nt(a, b):
    return lax.dot_general(a, b, (((1,), (1,)), ((), ())), preferred_element_type=F32)


def tn(a, b):
    return lax.dot_general(a, b, (((0,), (0,)), ((), ())), preferred_element_type=F32)


def nn(a, b):
    return lax.dot_general(a, b, (((1,), (0,)), ((), ())), preferred_element_type=F32)


def split(a):
    hi = a.astype(BF16)
    lo = (a - hi.astype(F32)).astype(BF16)
    return hi, lo


def kernel(h_ref, g_ref, xown_ref, pu_ref, pd_ref, m_ref, v_ref,
           w_out, m_out, v_out,
           xw, h0, g1, h1, g0, xo, pq, mv, vv,
           act0, act1, gp0, dz0, dz1,
           part, rd, lbuf, rbuf, mid,
           rr, rmid, rl, rrt, zq, zbuf, res,
           wst, mst, vst,
           loc_sem, w_send, w_recv, ag_send, ag_recv, rs_send, rs_recv, r_send, r_recv, z_send, z_recv, out_sem):
    model = h_ref.shape[1]
    rank = pu_ref.shape[2]
    tok = h_ref.shape[0]
    group = NC * NX * tok
    step_size = STEP_SCALE / rank ** 0.5
    me = lax.axis_index("data")
    core = lax.rem(me, NC)
    x = lax.rem(lax.div(me, NC), NX)
    y = lax.rem(lax.div(me, NC * NX), NY)
    z = lax.div(me, NC * NX * NY)

    def dev(zz, yy, xx, cc):
        return ((lax.rem(zz, NZ) * NY + lax.rem(yy, NY)) * NX + lax.rem(xx, NX)) * NC + cc

    partner = dev(z, y, x, 1 - core)
    nbr = {
        "xp": dev(z, y, x + 1, core), "xm": dev(z, y, x + NX - 1, core),
        "yp": dev(z, y + 1, x, core), "ym": dev(z, y + NY - 1, x, core),
        "zp": dev(z + 1, y, x, core), "zm": dev(z + NZ - 1, y, x, core),
    }
    zdev = [None] + [dev(z + k, y, x, core) for k in range(1, NZ)]

    def remote(src, dst, ssem, rsem, target):
        return pltpu.make_async_remote_copy(
            src_ref=src, dst_ref=dst, send_sem=ssem, recv_sem=rsem,
            device_id=(target,), device_id_type=pl.DeviceIdType.MESH)

    local = []

    def stage(src, dst):
        copy = pltpu.make_async_copy(src, dst, loc_sem.at[len(local)])
        copy.start()
        local.append(copy)

    for layer in (0, 1):
        stage(xown_ref.at[layer], xw.at[layer, 0])
    stage(h_ref, h0.at[0, 0])
    stage(g_ref, g1.at[0, 0])
    stage(xown_ref, xo)
    for layer in (0, 1):
        stage(pu_ref.at[layer], pq.at[layer, :, pl.ds(0, rank)])
        stage(pd_ref.at[layer], pq.at[layer, :, pl.ds(rank, rank)])
    stage(m_ref, mv)
    stage(v_ref, vv)

    barrier = pltpu.get_barrier_semaphore()
    cross = {"xp": dev(z, y, x + 1, 1 - core), "xm": dev(z, y, x + NX - 1, 1 - core)}
    partners = [partner] + list(nbr.values()) + list(cross.values())
    for target in partners:
        pl.semaphore_signal(barrier, inc=1, device_id=(target,), device_id_type=pl.DeviceIdType.MESH)
    pl.semaphore_wait(barrier, len(partners))
    for copy in local:
        copy.wait()

    def piece(layer, s, prt):
        first, columns, _, _ = PARTS[prt]
        return xw.at[layer, s, :, pl.ds(first, columns)]

    def w_step(event):
        _, kind, layer, prt, dy, dz, direction, ny, nz = event
        here = piece(layer, slot(dy, dz), prt)
        if kind == "wait":
            remote(here, here, w_send.at[layer, prt], w_recv.at[layer, prt, slot(dy, dz)], partner).wait_recv()
        else:
            remote(here, piece(layer, slot(ny, nz), prt), w_send.at[layer, prt],
                   w_recv.at[layer, prt, slot(ny, nz)], nbr[direction]).start()

    pending = list(ORDER)

    def pump(until):
        while pending and pending[0][0] <= until:
            w_step(pending.pop(0))

    def w_drain(layer):
        for prt, (first, columns, _, _) in enumerate(PARTS):
            ref = xw.at[layer, pl.ds(1, SLOTS - 1), :, pl.ds(first, columns)]
            remote(ref, ref, w_send.at[layer, prt], w_recv.at[layer, prt, 0], partner).wait_send()

    half = tok // 2
    drains = []

    class Gather:
        def __init__(self, buf, index):
            self.buf, self.index = buf, index

        def copy(self, k, src, dst, target):
            return remote(src, dst, ag_send.at[self.index, k], ag_recv.at[self.index, k], target)

        def go(self, k, src, dst, target):
            copy = self.copy(k, src, dst, target)
            copy.start()
            drains.append(copy)

        def arrived(self, k, ref):
            self.copy(k, ref, ref, partner).wait_recv()

        def start(self):
            b = self.buf
            self.go(0, b.at[0, 0], b.at[0, 3], nbr["xp"])
            self.go(1, b.at[0, 0], b.at[0, 1], nbr["xm"])
            self.go(2, b.at[0, 0], b.at[1, 0], partner)

        def middle(self):
            b = self.buf
            lo, hi = pl.ds(0, half), pl.ds(half, half)
            self.arrived(0, b.at[0, 3])
            self.go(3, b.at[0, 3, lo], b.at[0, 2, lo], nbr["xp"])
            self.go(7, b.at[0, 3, lo], b.at[1, 2, lo], cross["xp"])
            self.go(5, b.at[0, 3], b.at[1, 3], partner)
            self.arrived(1, b.at[0, 1])
            self.go(4, b.at[0, 1, hi], b.at[0, 2, hi], nbr["xm"])
            self.go(8, b.at[0, 1, hi], b.at[1, 2, hi], cross["xm"])
            self.go(6, b.at[0, 1], b.at[1, 1], partner)

        def finish(self):
            b = self.buf
            lo, hi = pl.ds(0, half), pl.ds(half, half)
            self.arrived(2, b.at[1, 0])
            self.arrived(5, b.at[1, 3])
            self.arrived(6, b.at[1, 1])
            self.arrived(3, b.at[0, 2, lo])
            self.arrived(4, b.at[0, 2, hi])
            self.arrived(7, b.at[1, 2, lo])
            self.arrived(8, b.at[1, 2, hi])

    class Reduce:
        def __init__(self, index):
            self.index = index

        def copy(self, k, src, dst, target):
            return remote(src, dst, rs_send.at[self.index, k], rs_recv.at[self.index, k], target)

        def go(self, k, src, dst, target):
            copy = self.copy(k, src, dst, target)
            copy.start()
            drains.append(copy)

        def arrived(self, k, ref):
            self.copy(k, ref, ref, partner).wait_recv()

        def to_partner(self):
            i = self.index
            for dx in (2, 1, 3, 0):
                self.go(dx, part.at[i, 1, dx], rd.at[i, dx], partner)

        def ring(self):
            i = self.index
            lo, hi = pl.ds(0, half), pl.ds(half, half)
            def add(dx):
                self.arrived(dx, rd.at[i, dx])
                part[i, 0, dx] = part[i, 0, dx] + rd[i, dx]

            add(2)
            self.go(4, part.at[i, 0, 2, lo], mid.at[i, lo], nbr["xp"])
            self.go(5, part.at[i, 0, 2, hi], mid.at[i, hi], nbr["xm"])
            add(1)
            self.go(6, part.at[i, 0, 1, hi], lbuf.at[i, hi], nbr["xp"])
            add(3)
            self.go(7, part.at[i, 0, 3, lo], rbuf.at[i, lo], nbr["xm"])
            add(0)

        def ring_second(self):
            i = self.index
            lo, hi = pl.ds(0, half), pl.ds(half, half)
            self.arrived(4, mid.at[i, lo])
            part[i, 0, 1, lo] = part[i, 0, 1, lo] + mid[i, lo]
            self.go(8, part.at[i, 0, 1, lo], lbuf.at[i, lo], nbr["xp"])
            self.arrived(5, mid.at[i, hi])
            part[i, 0, 3, hi] = part[i, 0, 3, hi] + mid[i, hi]
            self.go(9, part.at[i, 0, 3, hi], rbuf.at[i, hi], nbr["xm"])

        def total(self):
            i = self.index
            lo, hi = pl.ds(0, half), pl.ds(half, half)
            self.arrived(6, lbuf.at[i, hi])
            self.arrived(7, rbuf.at[i, lo])
            self.arrived(8, lbuf.at[i, lo])
            self.arrived(9, rbuf.at[i, hi])
            return part[i, 0, 0] + lbuf[i] + rbuf[i]

    class Scatter:
        def __init__(self, layer):
            self.layer = layer

        def copy(self, k, src, dst, target):
            return remote(src, dst, r_send.at[self.layer, k], r_recv.at[self.layer, k], target)

        def go(self, k, src, dst, target):
            copy = self.copy(k, src, dst, target)
            copy.start()
            drains.append(copy)

        def arrived(self, k, ref):
            self.copy(k, ref, ref, partner).wait_recv()

        def ring(self):
            i = self.layer
            lo, hi = pl.ds(0, NZ // 2), pl.ds(NZ // 2, NZ // 2)
            self.go(0, rr.at[i, 2, lo], rmid.at[i, lo], nbr["yp"])
            self.go(1, rr.at[i, 2, hi], rmid.at[i, hi], nbr["ym"])
            self.go(2, rr.at[i, 1, hi], rl.at[i, hi], nbr["yp"])
            self.go(3, rr.at[i, 3, lo], rrt.at[i, lo], nbr["ym"])

        def ring_second(self):
            i = self.layer
            lo, hi = pl.ds(0, NZ // 2), pl.ds(NZ // 2, NZ // 2)
            self.arrived(0, rmid.at[i, lo])
            rr[i, 1, lo] = rr[i, 1, lo] + rmid[i, lo]
            self.go(4, rr.at[i, 1, lo], rl.at[i, lo], nbr["yp"])
            self.arrived(1, rmid.at[i, hi])
            rr[i, 3, hi] = rr[i, 3, hi] + rmid[i, hi]
            self.go(5, rr.at[i, 3, hi], rrt.at[i, hi], nbr["ym"])

        def along_z(self):
            i = self.layer
            lo, hi = pl.ds(0, NZ // 2), pl.ds(NZ // 2, NZ // 2)
            self.arrived(2, rl.at[i, hi])
            self.arrived(3, rrt.at[i, lo])
            self.arrived(4, rl.at[i, lo])
            self.arrived(5, rrt.at[i, hi])
            zq[i] = rr[i, 0] + rl[i] + rrt[i]
            for k in (4, 3, 5, 2, 6, 1, 7):
                copy = remote(zq.at[i, k], zbuf.at[i, NZ - k], z_send.at[i, k], z_recv.at[i, NZ - k], zdev[k])
                copy.start()
                drains.append(copy)

        def total(self):
            i = self.layer
            out = zq[i, 0]
            for k in range(1, NZ):
                remote(zbuf.at[i, k], zbuf.at[i, k], z_send.at[i, k], z_recv.at[i, k], partner).wait_recv()
                out = out + zbuf[i, k]
            return out

    rows = SLOTS * ROWS
    CH = 640
    per = CH // ROWS

    def xrows(layer, i):
        return xw[layer, pl.ds(i * per, per)].reshape(CH, model)

    def row_in_slot():
        r = lax.broadcasted_iota(jnp.int32, (CH, group), 0)
        return lax.rem(r, ROWS)

    def chunks(body):
        def step(i, carry):
            body(i)
            return carry
        lax.fori_loop(0, rows // CH, step, 0)

    def gelu_pair(zt):
        sq = zt * zt
        t = jnp.tanh(GELU_C * (zt + GELU_A * (zt * sq)))
        half_one = 0.5 * (1.0 + t)
        value = zt * half_one
        slope = half_one + 0.5 * zt * (1.0 - t * t) * (GELU_C * (1.0 + 3.0 * GELU_A * sq))
        return value, slope

    def to_down(v):
        r = row_in_slot()
        keep = jnp.logical_and(r >= SHARE, r < 2 * SHARE)
        return jnp.where(keep, pltpu.roll(v, SHARE, 0), 0.0)

    def to_up(v):
        return pltpu.roll(v, CH - SHARE, 0)

    def mask_up(v):
        return jnp.where(row_in_slot() < SHARE, v, 0.0)

    def block(i):
        return pl.ds(pl.multiple_of(i * CH, CH), CH)

    def products(act_ref, layer, out_index):
        for cc in (1, 0):
            toks = pl.ds(cc * (group // 2), group // 2)
            lhs = act_ref[:, toks]
            part[out_index, cc] = tn(lhs, xw[layer].reshape(rows, model)).reshape(NX, tok, model)
            if cc == 1:
                Reduce(out_index).to_partner()

    def flat(ref):
        return ref[...].reshape(group, model)

    def project(layer, h_ref2, g_ref2):
        hp = nn(flat(h_ref2), pq[layer])[:, :rank]
        gq = nn(flat(g_ref2), pq[layer])[:, rank:]
        return jnp.concatenate(split(hp), axis=1), jnp.concatenate(split(gq), axis=1)

    done = [max(e[0] for e in ORDER if e[2] == layer) for layer in (0, 1)]
    gather_h, gather_g = Gather(h0, 0), Gather(g1, 1)
    pump(0.0)
    gather_h.start()
    gather_g.start()
    pump(4.0)
    gather_h.middle()
    pump(6.0)
    gather_g.middle()
    pump(9.0)
    gather_h.finish()
    gather_g.finish()
    pump(done[0])

    @chunks
    def _(i):
        zt = nt(xrows(0, i), flat(h0))
        value, slope = gelu_pair(zt)
        gp0[block(i), :] = slope
        act0[block(i), :] = to_down(value).astype(BF16)

    pump(done[0] + 1.3)
    products(act0, 0, 0)
    pump(done[0] + 2.5)
    reduce0 = Reduce(0)
    reduce0.ring()
    pump(done[0] + 5.0)
    reduce0.ring_second()
    pump(done[0] + 8.0)
    h1[0, 0] = (h0[0, 0].astype(F32) + reduce0.total()).astype(BF16)
    gather1 = Gather(h1, 2)
    gather1.start()
    pump(done[0] + 11.0)
    gather1.middle()
    pump(done[1])
    gather1.finish()

    @chunks
    def _(i):
        x2 = xrows(1, i)
        value, slope = gelu_pair(nt(x2, flat(h1)))
        act1[block(i), :] = to_down(value).astype(BF16)
        dpost = to_up(nt(x2, flat(g1)))
        dz1[block(i), :] = mask_up(slope * dpost).astype(BF16)

    products(dz1, 1, 1)
    reduce1 = Reduce(1)

    def projected(layer, dz_ref, act_ref, h_ref2, g_ref2):
        hp, gq = project(layer, h_ref2, g_ref2)

        @chunks
        def _(i):
            both = nn(dz_ref[block(i), :], hp) + nn(act_ref[block(i), :], gq)
            both = both[:, :rank] + both[:, rank:]
            both = both.reshape(per // NZ, NZ, ROWS, rank)
            rr[layer, pl.ds(i * (per // NZ), per // NZ)] = both

    reduce1.ring()
    reduce1.ring_second()
    g0[0, 0] = (g1[0, 0].astype(F32) + reduce1.total()).astype(BF16)
    gather0 = Gather(g0, 3)
    gather0.start()
    projected(1, dz1, act1, h1, g1)
    scatter1 = Scatter(1)
    scatter1.ring()
    gather0.middle()
    gather0.finish()

    @chunks
    def _(i):
        dpost = to_up(nt(xrows(0, i), flat(g0)))
        dz0[block(i), :] = mask_up(gp0[block(i), :] * dpost).astype(BF16)

    scatter1.ring_second()
    projected(0, dz0, act0, h0, g0)
    scatter0 = Scatter(0)
    scatter0.ring()
    scatter1.along_z()

    def update(layer, red):
        mom = BETA_ONE * mv[layer] + (1.0 - BETA_ONE) * red
        var = BETA_TWO * vv[layer] + (1.0 - BETA_TWO) * red * red
        direction = (mom / (1.0 - BETA_ONE ** STEP)) / (jnp.sqrt(var / (1.0 - BETA_TWO ** STEP)) + ADAM_EPS)
        mst[layer] = mom
        vst[layer] = var
        r = lax.broadcasted_iota(jnp.int32, (ROWS, rank), 0)
        up = jnp.where(r < SHARE, direction, 0.0)
        down = jnp.where(r >= SHARE, direction, 0.0)
        both = jnp.concatenate([up, down], axis=1)
        hi, lo = split(both)
        change = nt(jnp.concatenate([hi, lo], axis=0), pq[layer])
        change = change[:ROWS] + change[ROWS:]
        wst[layer] = (xo[layer].astype(F32) - step_size * change).astype(BF16)

    scatter0.ring_second()
    scatter0.along_z()
    update(1, scatter1.total())
    update(0, scatter0.total())

    outs = [(wst, w_out), (mst, m_out), (vst, v_out)]
    copies = [pltpu.make_async_copy(src, dst, out_sem.at[k]) for k, (src, dst) in enumerate(outs)]
    for copy in copies:
        copy.start()
    w_drain(0)
    w_drain(1)
    for copy in drains:
        copy.wait_send()
    for copy in copies:
        copy.wait()


def fused_step(act_in, grad_top, xown, proj_up, proj_down, mom, var):
    tok, model = act_in.shape
    layers, _, rank = proj_up.shape
    group = NC * NX * tok
    rows = SLOTS * ROWS
    dma = pltpu.SemaphoreType.DMA
    anyspace = pl.BlockSpec(memory_space=pl.ANY)
    vm = pltpu.VMEM
    blk = (NC, NX, tok, model)
    scratch = [
        vm((2, SLOTS, ROWS, model), BF16),
        vm(blk, BF16), vm(blk, BF16), vm(blk, BF16), vm(blk, BF16),
        vm((2, ROWS, model), BF16), vm((2, model, 2 * rank), BF16), vm((2, ROWS, rank), F32), vm((2, ROWS, rank), F32),
        vm((rows, group), BF16), vm((rows, group), BF16), vm((rows, group), F32), vm((rows, group), BF16), vm((rows, group), BF16),
        vm((2,) + blk, F32), vm((2, NX, tok, model), F32), vm((2, tok, model), F32), vm((2, tok, model), F32), vm((2, tok, model), F32),
        vm((2, NY, NZ, ROWS, rank), F32), vm((2, NZ, ROWS, rank), F32), vm((2, NZ, ROWS, rank), F32), vm((2, NZ, ROWS, rank), F32),
        vm((2, NZ, ROWS, rank), F32), vm((2, NZ, ROWS, rank), F32), vm((2, ROWS, rank), F32),
        vm((2, ROWS, model), BF16), vm((2, ROWS, rank), F32), vm((2, ROWS, rank), F32),
        dma((11,)), dma((2, len(PARTS))), dma((2, len(PARTS), SLOTS)), dma((4, 9)), dma((4, 9)), dma((2, 10)), dma((2, 10)),
        dma((2, 6)), dma((2, 6)), dma((2, NZ)), dma((2, NZ)), dma((3,)),
    ]
    return pl.pallas_call(
        kernel,
        name="galore_step",
        out_shape=(jax.ShapeDtypeStruct((2, ROWS, model), BF16), jax.ShapeDtypeStruct((2, ROWS, rank), F32),
                   jax.ShapeDtypeStruct((2, ROWS, rank), F32)),
        in_specs=[anyspace] * 7,
        out_specs=(anyspace,) * 3,
        scratch_shapes=scratch,
        compiler_params=pltpu.CompilerParams(collective_id=0, has_side_effects=True, vmem_limit_bytes=48 * 1024 * 1024),
    )(act_in, grad_top, xown, proj_up, proj_down, mom, var)


def solution(mesh):
    def pack(up, down):
        up = up.transpose(0, 2, 1)
        pad = jnp.zeros((up.shape[0], ROWS - 2 * SHARE, up.shape[2]), up.dtype)
        return jnp.concatenate([up, down, pad], axis=1)

    def unpack(packed):
        return packed[:, :SHARE].transpose(0, 2, 1), packed[:, SHARE:2 * SHARE]

    def device_step(act_in, grad_top, w_up, w_down, proj_up, proj_down, mom_up, var_up, mom_down, var_down):
        w_new, m_new, v_new = fused_step(act_in, grad_top, pack(w_up, w_down), proj_up, proj_down,
                                         pack(mom_up, mom_down), pack(var_up, var_down))
        new_up, new_down = unpack(w_new)
        new_mom_up, new_mom_down = unpack(m_new)
        new_var_up, new_var_down = unpack(v_new)
        return new_up, new_down, new_mom_up, new_var_up, new_mom_down, new_var_down

    tok_spec = P("data", None)
    col_spec = P(None, None, "data")
    row_spec = P(None, "data", None)
    return jax.shard_map(
        device_step,
        mesh=mesh,
        in_specs=(tok_spec, tok_spec, col_spec, row_spec, P(), P(), col_spec, col_spec, row_spec, row_spec),
        out_specs=(col_spec, row_spec, col_spec, col_spec, row_spec, row_spec),
        check_vma=False,
    )
```
